32 devices in a mesh: outer: 2 (over core), inner: 16 (over z, y, x).
Axes of the slice: x: 2, y: 2, z: 4, core: 2. Of those that a mesh axis runs over, the one named last changes fastest.
Arguments:
- inputs: float32 [50176, 256], P(('outer', 'inner')), may hold values from -6 to 6
- cotangent: float32 [50176, 1024], P(('outer', 'inner')), may hold values from -200 to 200
- weight: float32 [1024, 256], replicated, may hold values from -0.375 to 0.375
- momentum: float32 [1024, 256], P('inner', 'outer'), may hold values from -4 to 4
Outputs:
- input_grad: float32 [50176, 256], P(('outer', 'inner'))
- new_weight: float32 [1024, 256], P(None, 'outer')
- new_momentum: float32 [1024, 256], P('inner', 'outer')
The draws below stay inside these ranges and needn't reach their ends.
All inputs are finite; a program needn't handle non-finite values.
Results may differ from the reference program's by a relative error of at most 0.0001.
Values sent between devices are 32-bit elements; how exact they have to be, the bound alone decides.
A program may use at most 64 MiB of HBM per device.

```python
import jax
import jax.numpy as jnp
from jax import lax

CIN = 256
COUT = 1024
TOKENS = 50176
N_OUTER = 2


def draw_inputs(key, part):
    first = jax.random.fold_in(key, 11)
    second = jax.random.fold_in(key, 12)
    third = jax.random.fold_in(key, 13)
    shared = 0.5 * jnp.clip(jax.random.normal(first, (1, CIN), jnp.float32), -2.5, 2.5)
    own = 0.5 * jnp.clip(jax.random.normal(third, (N_OUTER, CIN), jnp.float32), -2.5, 2.5)
    centre = 0.8 * shared + 0.6 * own
    noise = jnp.clip(jax.random.normal(second, (TOKENS, CIN), jnp.float32), -4.0, 4.0)
    grouped = noise.reshape(N_OUTER, TOKENS // N_OUTER, CIN) + centre[:, None, :]
    return grouped.reshape(TOKENS, CIN)


def draw_cotangent(key, part):
    first = jax.random.fold_in(key, 21)
    second = jax.random.fold_in(key, 22)
    third = jax.random.fold_in(key, 23)
    fourth = jax.random.fold_in(key, 24)
    fifth = jax.random.fold_in(key, 25)
    shared = jnp.clip(jax.random.normal(first, (1, COUT), jnp.float32), -2.5, 2.5)
    own = jnp.clip(jax.random.normal(fifth, (N_OUTER, COUT), jnp.float32), -2.5, 2.5)
    centre = 0.5 * shared + 0.5 * own
    ramp = jnp.exp(jnp.log(3.0) * jnp.arange(COUT, dtype=jnp.float32) / COUT)
    rough = jnp.exp(jax.random.uniform(second, (COUT,), jnp.float32, 0.0, jnp.log(4.0)))
    row_scale = jnp.exp(jax.random.uniform(third, (TOKENS, 1), jnp.float32, 0.0, jnp.log(10.0)))
    noise = jnp.clip(jax.random.normal(fourth, (TOKENS, COUT), jnp.float32), -4.0, 4.0)
    grouped = noise.reshape(N_OUTER, TOKENS // N_OUTER, COUT) + centre[:, None, :]
    return 0.25 * grouped.reshape(TOKENS, COUT) * (ramp * rough)[None, :] * row_scale


def block_levels(stream_key, extent, split, smallest, high):
    loudness = 1.0
    for position, parts in split:
        heights = jax.random.uniform(jax.random.fold_in(jax.random.fold_in(stream_key, 6), position), (parts,), jnp.float32, smallest / len(split), high / len(split))
        loudness = loudness * jnp.repeat(jnp.exp(heights), extent[position] // parts).reshape((-1,) + (1,) * (len(extent) - 1 - position))
    return loudness


def scatter_about(key, extent, scale, most, cuts=(), held_as=jnp.bfloat16):
    array = scale * jax.random.normal(key, extent, jnp.float32)
    if cuts:
        array = array * block_levels(key, extent, cuts, -0.22, 0.18)
    return jnp.clip(array, -most, most).astype(held_as)


def setup_inputs(seed: int = 0) -> dict:
    key_of = jax.random.split(jax.random.key(seed), 5)
    inputs = draw_inputs(jax.random.fold_in(key_of[4], 71), 0)
    cotangent = draw_cotangent(jax.random.fold_in(key_of[4], 71), 0)
    weight = scatter_about(key_of[2], (COUT, CIN), CIN ** -0.5, 0.375, (), jnp.float32)
    momentum = scatter_about(key_of[3], (COUT, CIN), 0.3, 4.0, ((0, 16), (1, 2)), jnp.float32)
    return {"inputs": inputs, "cotangent": cotangent, "weight": weight, "momentum": momentum}


HIGH = lax.Precision.HIGHEST

def adasum_pair(first, second):
    cross = jnp.sum(first * second)
    first_sq = jnp.sum(first * first)
    second_sq = jnp.sum(second * second)
    return (1.0 - cross / (2.0 * (first_sq + 1e-06))) * first + (1.0 - cross / (2.0 * (second_sq + 1e-06))) * second

def reference(inputs, cotangent, weight, momentum):
    pre = jnp.dot(inputs, weight.T, precision=HIGH, preferred_element_type=jnp.float32)
    sig = jax.nn.sigmoid(pre)
    slope = cotangent * (sig * (1.0 + pre * (1.0 - sig)))
    input_grad = jnp.dot(slope, weight, precision=HIGH, preferred_element_type=jnp.float32)
    group_rows = inputs.shape[0] // N_OUTER
    xs = inputs.reshape(N_OUTER, group_rows, CIN)
    slopes = slope.reshape(N_OUTER, group_rows, COUT)

    def group_grad(pair):
        return jnp.dot(pair[0].T, pair[1], precision=HIGH, preferred_element_type=jnp.float32) * (1.0 / group_rows)
    grads = lax.map(group_grad, (slopes, xs))
    levels = N_OUTER.bit_length() - 1
    for level in range(levels):
        paired = grads.reshape(grads.shape[0] // 2, 2, COUT, CIN)
        grads = jax.vmap(adasum_pair)(paired[:, 0], paired[:, 1])
    combined = grads[0]
    new_momentum = 0.9 * momentum + combined
    new_weight = weight - 0.1 * new_momentum
    return (input_grad, new_weight, new_momentum)
```

```python
import functools

import jax
import jax.numpy as jnp
from jax import lax
from jax.experimental import pallas as pl
from jax.experimental.pallas import tpu as pltpu
from jax.sharding import PartitionSpec as P

MESH = pl.DeviceIdType.MESH
F32 = jnp.float32
BF16 = jnp.bfloat16


def split(value):
    high = value.astype(BF16)
    return high, (value - high.astype(F32)).astype(BF16)


def dot(a, b):
    return jnp.dot(a, b, preferred_element_type=F32)


def dot_t(a, b):
    return lax.dot_general(a, b, (((1,), (1,)), ((), ())), preferred_element_type=F32)


def row_tile(rows):
    best = 16
    for size in range(16, 257, 16):
        if rows % size == 0:
            best = size
    return best


def planes_of(inner):
    for planes in (4, 2):
        if inner % planes == 0:
            return planes
    return 1


def kernel(
    n_inner, planes, scale,
    x_ref, cot_hbm, w_ref, mom_ref,
    ig_hbm, nw_ref, nm_ref,
    cot, xcat, xt_hi, xt_lo, wcat, s_hi, s_lo, ig, send1, recv1, send2, recv2, final, stat, stats, nw,
    cot_sem, ig_sem, ssem1, rsem1, ssem2, rsem2, ssem3, rsem3, ssem4, rsem4, ssem5,
):
    o = lax.axis_index("outer")
    i = lax.axis_index("inner")
    side = n_inner // planes
    z = i // side
    j = i % side
    rows, cin = x_ref.shape
    cout = w_ref.shape[0]
    width = cout // planes
    own = cout // n_inner
    half = cin // 2
    tile = row_tile(rows)
    tiles = rows // tile

    def plane_of(c):
        return lax.rem(z + 1 + c, planes)

    def cot_copy(c):
        k = plane_of(c)
        return pltpu.make_async_copy(
            cot_hbm.at[:, pl.ds(pl.multiple_of(k * width, width), width)], cot.at[c], cot_sem.at[c]
        )

    for c in range(planes):
        cot_copy(c).start()

    barrier = pltpu.get_barrier_semaphore()
    n_all = 2 * n_inner

    for e in range(2):

        def greet(d, _, e=e):
            @pl.when((d + e) > 0)
            def _():
                pl.semaphore_signal(
                    barrier, inc=1,
                    device_id=(lax.rem(o + e, 2), lax.rem(i + d, n_inner)), device_id_type=MESH,
                )
            return 0

        lax.fori_loop(0, n_inner, greet, 0)

    for t in range(tiles):
        at = pl.ds(t * tile, tile)
        block = x_ref[at, :]
        high, low = split(block)
        xcat[at, 0:cin] = high
        xcat[at, cin : 2 * cin] = low
        xcat[at, 2 * cin : 3 * cin] = high
        block_t = block.T
        high_t, low_t = split(block_t)
        xt_hi[t] = high_t
        xt_lo[t] = low_t
    high, low = split(w_ref[...])
    wcat[:, 0:cin] = high
    wcat[:, cin : 2 * cin] = high
    wcat[:, 2 * cin : 3 * cin] = low

    def piece_copy(c, e, d):
        other = lax.rem(o + e, 2)
        target = lax.rem(j + d, side)
        return pltpu.make_async_remote_copy(
            src_ref=send1.at[c, other, target],
            dst_ref=recv1.at[c, o, j],
            send_sem=ssem1.at[c, e, d],
            recv_sem=rsem1.at[c, o, j],
            device_id=(other, z * side + target),
            device_id_type=MESH,
        )

    def piece_arrival(c, e, d):
        g = lax.rem(o + e, 2)
        source = lax.rem(j + side - d, side)
        return pltpu.make_async_remote_copy(
            src_ref=recv1.at[c, g, source],
            dst_ref=recv1.at[c, g, source],
            send_sem=ssem1.at[c, e, d],
            recv_sem=rsem1.at[c, g, source],
            device_id=(g, z * side + source),
            device_id_type=MESH,
        )

    pieces = [(e, d) for d in range(side) for e in range(2) if (e, d) != (0, 0)]

    def plane_copy(c):
        return pltpu.make_async_remote_copy(
            src_ref=send2.at[c],
            dst_ref=recv2.at[c],
            send_sem=ssem2.at[c],
            recv_sem=rsem2.at[c],
            device_id=(o, plane_of(c) * side + j),
            device_id_type=MESH,
        )

    def gather_plane(c):
        for e, d in pieces:
            piece_arrival(c, e, d).wait_recv()
        total = recv1[c, :, 0]
        for source in range(1, side):
            total = total + recv1[c, :, source]
        return total

    def compute(c):
        k = plane_of(c)
        cot_copy(c).wait()
        w_at = pl.ds(pl.multiple_of(k * width, width), width)
        w_k = wcat[w_at, :]

        def pre_of(t):
            return dot_t(xcat[t * tile : (t + 1) * tile, :], w_k)

        pre_next = pre_of(0)
        acc = jnp.zeros((cin, width), F32)
        for t in range(tiles):
            pre = pre_next
            if t + 1 < tiles:
                pre_next = pre_of(t + 1)
            at = pl.ds(t * tile, tile)
            sig = 1.0 / (1.0 + jnp.exp(-pre))
            slope = cot[c, at, :] * (sig * (1.0 + pre * (1.0 - sig)))
            high, low = split(slope)
            s_hi[k, at, :] = high
            s_lo[k, at, :] = low
            acc = acc + (dot(xt_hi[t], high) + dot(xt_hi[t], low) + dot(xt_lo[t], high))
        grad = acc.T * scale
        for h in range(2):
            send1[c, h] = grad[:, h * half : (h + 1) * half].reshape(side, own, half)

    def chunk(c, _):
        compute(c)

        @pl.when(c == 0)
        def _():
            pl.semaphore_wait(barrier, n_all - 1)

        for e, d in pieces:
            piece_copy(c, e, d).start()
        recv1[c, o, j] = send1[c, o, j]

        @pl.when(c > 0)
        def _():
            send2[c - 1] = gather_plane(c - 1)
            plane_copy(c - 1).start()

        return 0

    lax.fori_loop(0, planes, chunk, 0)

    def input_grad(t):
        at = pl.ds(t * tile, tile)
        total = jnp.zeros((tile, cin), F32)
        for k in range(planes):
            w_at = pl.ds(k * width, width)
            w_hi = wcat[w_at, 0:cin]
            total = total + dot(s_hi[k, at, :], w_hi) + dot(s_lo[k, at, :], w_hi)
            total = total + dot(s_hi[k, at, :], wcat[w_at, 2 * cin : 3 * cin])
        ig[at, :] = total
        pltpu.make_async_copy(ig.at[at, :], ig_hbm.at[at, :], ig_sem.at[t]).start()

    early = tiles // 2 + 1
    for t in range(early):
        input_grad(t)

    total = gather_plane(planes - 1)
    for c in range(planes - 1):
        plane_copy(c).wait_recv()
        total = total + recv2[c]
    final[...] = total
    first, second = total[0], total[1]

    me = o * n_inner + i
    rows_of = [
        jnp.sum(value, axis=0, keepdims=True)
        for value in (first * second, first * first, second * second)
    ]
    stat[...] = jnp.concatenate(rows_of + [jnp.zeros((5, half), F32)], axis=0)
    stats[me] = stat[...]

    def stat_copy(e, d):
        other = lax.rem(o + e, 2)
        target = lax.rem(i + d, n_inner)
        return pltpu.make_async_remote_copy(
            src_ref=stat,
            dst_ref=stats.at[me],
            send_sem=ssem3.at[e, d],
            recv_sem=rsem3.at[me],
            device_id=(other, target),
            device_id_type=MESH,
        )

    def stat_arrival(e, d):
        g = lax.rem(o + e, 2)
        source = lax.rem(i + n_inner - d, n_inner)
        return pltpu.make_async_remote_copy(
            src_ref=stat,
            dst_ref=stats.at[g * n_inner + source],
            send_sem=ssem3.at[e, d],
            recv_sem=rsem3.at[g * n_inner + source],
            device_id=(g, source),
            device_id_type=MESH,
        )

    everybody = [(e, d) for d in range(n_inner) for e in range(2) if (e, d) != (0, 0)]
    for e, d in everybody:
        stat_copy(e, d).start()

    for t in range(early, tiles):
        input_grad(t)

    for e, d in everybody:
        stat_arrival(e, d).wait_recv()
    sums = jnp.sum(jnp.sum(stats[...], axis=0), axis=1, keepdims=True)
    cross, first_sq, second_sq = sums[0:1], sums[1:2], sums[2:3]
    combined = (1.0 - cross / (2.0 * (first_sq + 1e-06))) * final[0] + (
        1.0 - cross / (2.0 * (second_sq + 1e-06))
    ) * final[1]
    momentum = 0.9 * mom_ref[...] + combined
    nm_ref[...] = momentum
    w_rows = w_ref[pl.ds(pl.multiple_of(i * own, own), own), :]
    w_own = jnp.where(o == 0, w_rows[:, 0:half], w_rows[:, half : 2 * half])
    nw[i] = w_own - 0.1 * momentum

    def filter_copy(block, target, send_sem):
        return pltpu.make_async_remote_copy(
            src_ref=nw.at[block],
            dst_ref=nw.at[block],
            send_sem=send_sem,
            recv_sem=rsem4.at[block],
            device_id=(o, target),
            device_id_type=MESH,
        )

    for p in range(1, planes):
        filter_copy(i, lax.rem(z + p, planes) * side + j, ssem4.at[p]).start()
    order = [0]
    for p in range(1, planes // 2 + 1):
        order += [p] if p == planes - p else [p, planes - p]
    for p in order:
        block = lax.rem(z + planes - p, planes) * side + j
        if p:
            filter_copy(block, i, ssem4.at[p]).wait_recv()
        for d in range(1, side):
            filter_copy(block, z * side + lax.rem(j + d, side), ssem5.at[p, d]).start()
    for p in range(planes):
        for d in range(1, side):
            block = lax.rem(z + planes - p, planes) * side + lax.rem(j + d, side)
            filter_copy(block, i, ssem5.at[p, d]).wait_recv()
    nw_ref[...] = nw[...]

    for t in range(tiles):
        at = pl.ds(t * tile, tile)
        pltpu.make_async_copy(ig.at[at, :], ig_hbm.at[at, :], ig_sem.at[t]).wait()
    for c in range(planes):
        for e, d in pieces:
            piece_copy(c, e, d).wait_send()
        if c < planes - 1:
            plane_copy(c).wait_send()
    for e, d in everybody:
        stat_copy(e, d).wait_send()
    for p in range(planes):
        if p:
            filter_copy(i, lax.rem(z + p, planes) * side + j, ssem4.at[p]).wait_send()
        block = lax.rem(z + planes - p, planes) * side + j
        for d in range(1, side):
            filter_copy(block, z * side + lax.rem(j + d, side), ssem5.at[p, d]).wait_send()


def solution(mesh):
    n_inner = mesh.shape["inner"]
    planes = planes_of(n_inner)
    side = n_inner // planes

    def per_device(inputs, cotangent, weight, momentum):
        rows, cin = inputs.shape
        cout = weight.shape[0]
        own, half = momentum.shape
        width = cout // planes
        tile = row_tile(rows)
        tiles = rows // tile
        dma = pltpu.SemaphoreType.DMA
        vmem = pl.BlockSpec(memory_space=pltpu.VMEM)
        hbm = pl.BlockSpec(memory_space=pl.ANY)
        input_grad, new_weight, new_momentum = pl.pallas_call(
            functools.partial(kernel, n_inner, planes, 1.0 / (rows * n_inner)),
            out_shape=(
                jax.ShapeDtypeStruct((rows, cin), F32),
                jax.ShapeDtypeStruct((n_inner, own, half), F32),
                jax.ShapeDtypeStruct((own, half), F32),
            ),
            in_specs=[vmem, hbm, vmem, vmem],
            out_specs=(hbm, vmem, vmem),
            scratch_shapes=[
                pltpu.VMEM((planes, rows, width), F32),
                pltpu.VMEM((rows, 3 * cin), BF16),
                pltpu.VMEM((tiles, cin, tile), BF16),
                pltpu.VMEM((tiles, cin, tile), BF16),
                pltpu.VMEM((cout, 3 * cin), BF16),
                pltpu.VMEM((planes, rows, width), BF16),
                pltpu.VMEM((planes, rows, width), BF16),
                pltpu.VMEM((rows, cin), F32),
                pltpu.VMEM((planes, 2, side, own, half), F32),
                pltpu.VMEM((planes, 2, side, own, half), F32),
                pltpu.VMEM((planes, 2, own, half), F32),
                pltpu.VMEM((planes, 2, own, half), F32),
                pltpu.VMEM((2, own, half), F32),
                pltpu.VMEM((8, half), F32),
                pltpu.VMEM((2 * n_inner, 8, half), F32),
                pltpu.VMEM((n_inner, own, half), F32),
                dma((planes,)),
                dma((tiles,)),
                dma((planes, 2, side)),
                dma((planes, 2, side)),
                dma((planes,)),
                dma((planes,)),
                dma((2, n_inner)),
                dma((2 * n_inner,)),
                dma((planes,)),
                dma((n_inner,)),
                dma((planes, side)),
            ],
            compiler_params=pltpu.CompilerParams(
                collective_id=0, has_side_effects=True, vmem_limit_bytes=60 * 1024 * 1024
            ),
            name="adasum_step",
        )(inputs, cotangent, weight, momentum)
        return input_grad, new_weight.reshape(cout, half), new_momentum

    placed = (P(("outer", "inner"), None), P(("outer", "inner"), None), P(), P("inner", "outer"))
    return jax.shard_map(
        per_device,
        mesh=mesh,
        in_specs=placed,
        out_specs=(P(("outer", "inner"), None), P(None, "outer"), P("inner", "outer")),
        check_vma=False,
    )
```

```python
import functools

import jax
import jax.numpy as jnp
from jax import lax
from jax.experimental import pallas as pl
from jax.experimental.pallas import tpu as pltpu
from jax.sharding import PartitionSpec as P

MESH = pl.DeviceIdType.MESH
F32 = jnp.float32
BF16 = jnp.bfloat16


def split(value):
    high = value.astype(BF16)
    return high, (value - high.astype(F32)).astype(BF16)


def dot(a, b):
    return jnp.dot(a, b, preferred_element_type=F32)


def dot_t(a, b):
    return lax.dot_general(a, b, (((1,), (1,)), ((), ())), preferred_element_type=F32)


def row_tile(rows):
    best = 16
    for size in range(16, 257, 16):
        if rows % size == 0:
            best = size
    return best


def planes_of(inner):
    for planes in (4, 2):
        if inner % planes == 0:
            return planes
    return 1


def kernel(
    n_inner, planes, scale,
    x_ref, cot_hbm, w_ref, mom_ref,
    ig, nw_ref, nm_ref,
    cot, xcat, xt_hi, xt_lo, wcat, s_hi, s_lo, send1, recv1, send2, recv2, raw, moms, stat, stats, nw,
    cot_sem, ssem1, rsem1, ssem2, rsem2, ssem3, rsem3, ssem4, rsem4, ssem5, rsem5, ssem6, rsem6, ssem7, rsem7,
):
    o = lax.axis_index("outer")
    i = lax.axis_index("inner")
    side = n_inner // planes
    z = i // side
    j = i % side
    rows, cin = x_ref.shape
    cout = w_ref.shape[0]
    width = cout // planes
    own = cout // n_inner
    half = cin // 2
    tile = row_tile(rows)
    tiles = rows // tile

    def plane_of(c):
        return lax.rem(z + 1 + c, planes)

    def cot_copy(c):
        k = plane_of(c)
        return pltpu.make_async_copy(
            cot_hbm.at[:, pl.ds(pl.multiple_of(k * width, width), width)], cot.at[c], cot_sem.at[c]
        )

    for c in range(planes):
        cot_copy(c).start()

    barrier = pltpu.get_barrier_semaphore()
    n_all = 2 * n_inner

    for e in range(2):

        def greet(d, _, e=e):
            @pl.when((d + e) > 0)
            def _():
                pl.semaphore_signal(
                    barrier, inc=1,
                    device_id=(lax.rem(o + e, 2), lax.rem(i + d, n_inner)), device_id_type=MESH,
                )
            return 0

        lax.fori_loop(0, n_inner, greet, 0)

    for t in range(tiles):
        at = pl.ds(t * tile, tile)
        block = x_ref[at, :]
        high, low = split(block)
        xcat[at, 0:cin] = high
        xcat[at, cin : 2 * cin] = low
        xcat[at, 2 * cin : 3 * cin] = high
        block_t = block.T
        high_t, low_t = split(block_t)
        xt_hi[t] = high_t
        xt_lo[t] = low_t
    high, low = split(w_ref[...])
    wcat[:, 0:cin] = high
    wcat[:, cin : 2 * cin] = high
    wcat[:, 2 * cin : 3 * cin] = low

    def piece_copy(c, e, d):
        other = lax.rem(o + e, 2)
        target = lax.rem(j + d, side)
        return pltpu.make_async_remote_copy(
            src_ref=send1.at[c, other, target],
            dst_ref=recv1.at[c, o, j],
            send_sem=ssem1.at[c, e, d],
            recv_sem=rsem1.at[c, o, j],
            device_id=(other, z * side + target),
            device_id_type=MESH,
        )

    def piece_arrival(c, e, d):
        g = lax.rem(o + e, 2)
        source = lax.rem(j + side - d, side)
        return pltpu.make_async_remote_copy(
            src_ref=recv1.at[c, g, source],
            dst_ref=recv1.at[c, g, source],
            send_sem=ssem1.at[c, e, d],
            recv_sem=rsem1.at[c, g, source],
            device_id=(g, z * side + source),
            device_id_type=MESH,
        )

    pieces = [(e, d) for d in range(side) for e in range(2) if (e, d) != (0, 0)]

    def plane_copy(c):
        return pltpu.make_async_remote_copy(
            src_ref=send2.at[c],
            dst_ref=recv2.at[c],
            send_sem=ssem2.at[c],
            recv_sem=rsem2.at[c],
            device_id=(o, plane_of(c) * side + j),
            device_id_type=MESH,
        )

    def gather_plane(c):
        for e, d in pieces:
            piece_arrival(c, e, d).wait_recv()
        total = recv1[c, :, 0]
        for source in range(1, side):
            total = total + recv1[c, :, source]
        return total

    def line_copy(array, p, ssem, rsem):
        return pltpu.make_async_remote_copy(
            src_ref=array.at[z],
            dst_ref=array.at[z],
            send_sem=ssem.at[p],
            recv_sem=rsem.at[z],
            device_id=(o, lax.rem(z + p, planes) * side + j),
            device_id_type=MESH,
        )

    def line_arrival(array, p, ssem, rsem):
        source = lax.rem(z + planes - p, planes)
        return pltpu.make_async_remote_copy(
            src_ref=array.at[source],
            dst_ref=array.at[source],
            send_sem=ssem.at[p],
            recv_sem=rsem.at[source],
            device_id=(o, source * side + j),
            device_id_type=MESH,
        )

    moms[z] = mom_ref[...]

    def compute(c):
        k = plane_of(c)
        cot_copy(c).wait()
        w_at = pl.ds(pl.multiple_of(k * width, width), width)
        w_k = wcat[w_at, :]

        def pre_of(t):
            return dot_t(xcat[t * tile : (t + 1) * tile, :], w_k)

        pre_next = pre_of(0)
        acc = jnp.zeros((cin, width), F32)
        for t in range(tiles):
            pre = pre_next
            if t + 1 < tiles:
                pre_next = pre_of(t + 1)
            at = pl.ds(t * tile, tile)
            sig = 1.0 / (1.0 + jnp.exp(-pre))
            slope = cot[c, at, :] * (sig * (1.0 + pre * (1.0 - sig)))
            high, low = split(slope)
            s_hi[k, at, :] = high
            s_lo[k, at, :] = low
            acc = acc + (dot(xt_hi[t], high) + dot(xt_hi[t], low) + dot(xt_lo[t], high))
        grad = acc.T * scale
        for h in range(2):
            send1[c, h] = grad[:, h * half : (h + 1) * half].reshape(side, own, half)

    def chunk(c, _):
        compute(c)

        @pl.when(c == 0)
        def _():
            pl.semaphore_wait(barrier, n_all - 1)

        for e, d in pieces:
            piece_copy(c, e, d).start()
        recv1[c, o, j] = send1[c, o, j]

        @pl.when(c == 0)
        def _():
            for p in range(1, planes):
                line_copy(moms, p, ssem6, rsem6).start()

        @pl.when(c > 0)
        def _():
            send2[c - 1] = gather_plane(c - 1)
            plane_copy(c - 1).start()

        return 0

    lax.fori_loop(0, planes, chunk, 0)

    def input_grad(t):
        at = pl.ds(t * tile, tile)
        total = jnp.zeros((tile, cin), F32)
        for k in range(planes):
            w_at = pl.ds(k * width, width)
            w_hi = wcat[w_at, 0:cin]
            total = total + dot(s_hi[k, at, :], w_hi) + dot(s_lo[k, at, :], w_hi)
            total = total + dot(s_hi[k, at, :], wcat[w_at, 2 * cin : 3 * cin])
        ig[at, :] = total

    early = tiles // 2 + 1
    for t in range(early):
        input_grad(t)

    total = gather_plane(planes - 1)
    for c in range(planes - 1):
        plane_copy(c).wait_recv()
        total = total + recv2[c]
    raw[z] = total
    first, second = total[0], total[1]

    me = o * n_inner + i
    rows_of = [
        jnp.sum(value, axis=0, keepdims=True)
        for value in (first * second, first * first, second * second)
    ]
    stat[...] = jnp.concatenate(rows_of + [jnp.zeros((5, half), F32)], axis=0)
    stats[me] = stat[...]

    def stat_copy(e, d):
        other = lax.rem(o + e, 2)
        target = lax.rem(i + d, n_inner)
        return pltpu.make_async_remote_copy(
            src_ref=stat,
            dst_ref=stats.at[me],
            send_sem=ssem3.at[e, d],
            recv_sem=rsem3.at[me],
            device_id=(other, target),
            device_id_type=MESH,
        )

    def stat_arrival(e, d):
        g = lax.rem(o + e, 2)
        source = lax.rem(i + n_inner - d, n_inner)
        return pltpu.make_async_remote_copy(
            src_ref=stat,
            dst_ref=stats.at[g * n_inner + source],
            send_sem=ssem3.at[e, d],
            recv_sem=rsem3.at[g * n_inner + source],
            device_id=(g, source),
            device_id_type=MESH,
        )

    everybody = [(e, d) for d in range(n_inner) for e in range(2) if (e, d) != (0, 0)]
    for e, d in everybody:
        stat_copy(e, d).start()
    for p in range(1, planes):
        line_copy(raw, p, ssem4, rsem5).start()

    for t in range(early, tiles):
        input_grad(t)

    for e, d in everybody:
        stat_arrival(e, d).wait_recv()
    sums = jnp.sum(jnp.sum(stats[...], axis=0), axis=1, keepdims=True)
    cross, first_sq, second_sq = sums[0:1], sums[1:2], sums[2:3]
    first_by = 1.0 - cross / (2.0 * (first_sq + 1e-06))
    second_by = 1.0 - cross / (2.0 * (second_sq + 1e-06))

    def filter_copy(block, at, target, send_sem, recv_sem):
        return pltpu.make_async_remote_copy(
            src_ref=nw.at[block, at],
            dst_ref=nw.at[block, at],
            send_sem=send_sem,
            recv_sem=recv_sem,
            device_id=(o, z * side + target),
            device_id_type=MESH,
        )

    def plane_back(p):
        return lax.rem(z + planes - p, planes)

    whole = pl.ds(0, own)
    square = side == 4 and own % 16 == 0
    across = j + 1 - 2 * lax.rem(j, 2)
    along = j + 2 - 4 * (j // 2)
    targets = (across, along) if square else tuple(lax.rem(j + d, side) for d in range(1, side))
    sources = targets if square else tuple(lax.rem(j + side - d, side) for d in range(1, side))
    low_rows, high_rows = pl.ds(0, own // 2), pl.ds(own // 2, own // 2)

    def block_copies(p):
        block = plane_back(p) * side + j
        return [
            filter_copy(block, whole, target, ssem5.at[p, d], rsem4.at[block])
            for d, target in enumerate(targets)
        ]

    def block_arrival(p, d):
        block = plane_back(p) * side + sources[d]
        return filter_copy(block, whole, j, ssem5.at[p, d], rsem4.at[block])

    def forward_copies(p):
        q = plane_back(p)
        return [
            filter_copy(q * side + across, low_rows, along, ssem7.at[p, 0], rsem7.at[q, 0]),
            filter_copy(q * side + along, high_rows, across, ssem7.at[p, 1], rsem7.at[q, 1]),
        ]

    def forward(p):
        for d, copy in enumerate(forward_copies(p)):
            block_arrival(p, d).wait_recv()
            copy.start()

    order = [0]
    for p in range(1, planes // 2 + 1):
        order += [p] if p == planes - p else [p, planes - p]
    for at, p in enumerate(order):
        q = plane_back(p)
        if p:
            line_arrival(moms, p, ssem6, rsem6).wait_recv()
            line_arrival(raw, p, ssem4, rsem5).wait_recv()
        momentum = 0.9 * moms[q] + (first_by * raw[q, 0] + second_by * raw[q, 1])
        if p == 0:
            nm_ref[...] = momentum
        block = q * side + j
        w_rows = w_ref[pl.ds(pl.multiple_of(block * own, own), own), :]
        w_own = jnp.where(o == 0, w_rows[:, 0:half], w_rows[:, half : 2 * half])
        nw[block] = w_own - 0.1 * momentum
        for copy in block_copies(p):
            copy.start()
        if square and at:
            forward(order[at - 1])
    if square:
        forward(order[-1])
    for p in order:
        q = plane_back(p)
        if square:
            for d, at in enumerate((low_rows, high_rows)):
                filter_copy(q * side + (side - 1 - j), at, j, ssem7.at[p, d], rsem7.at[q, d]).wait_recv()
        else:
            for d in range(len(sources)):
                block_arrival(p, d).wait_recv()
    nw_ref[...] = nw[...]

    for c in range(planes):
        for e, d in pieces:
            piece_copy(c, e, d).wait_send()
        if c < planes - 1:
            plane_copy(c).wait_send()
    for e, d in everybody:
        stat_copy(e, d).wait_send()
    for p in range(planes):
        if p:
            line_copy(moms, p, ssem6, rsem6).wait_send()
            line_copy(raw, p, ssem4, rsem5).wait_send()
        for copy in block_copies(p):
            copy.wait_send()
        if square:
            for copy in forward_copies(p):
                copy.wait_send()


def store_kernel(a, b, c, a_out, b_out, c_out, sems):
    copies = [
        pltpu.make_async_copy(source, target, sems.at[n])
        for n, (source, target) in enumerate(((a, a_out), (b, b_out), (c, c_out)))
    ]
    for copy in copies:
        copy.start()
    for copy in copies:
        copy.wait()


def solution(mesh):
    n_inner = mesh.shape["inner"]
    planes = planes_of(n_inner)
    side = n_inner // planes

    def per_device(inputs, cotangent, weight, momentum):
        rows, cin = inputs.shape
        cout = weight.shape[0]
        own, half = momentum.shape
        width = cout // planes
        tile = row_tile(rows)
        tiles = rows // tile
        dma = pltpu.SemaphoreType.DMA
        vmem = pl.BlockSpec(memory_space=pltpu.VMEM)
        hbm = pl.BlockSpec(memory_space=pl.ANY)
        input_grad, new_weight, new_momentum = pl.pallas_call(
            functools.partial(kernel, n_inner, planes, 1.0 / (rows * n_inner)),
            out_shape=(
                pltpu.VMEM((rows, cin), F32),
                pltpu.VMEM((n_inner, own, half), F32),
                pltpu.VMEM((own, half), F32),
            ),
            in_specs=[vmem, hbm, vmem, vmem],
            out_specs=(vmem, vmem, vmem),
            scratch_shapes=[
                pltpu.VMEM((planes, rows, width), F32),
                pltpu.VMEM((rows, 3 * cin), BF16),
                pltpu.VMEM((tiles, cin, tile), BF16),
                pltpu.VMEM((tiles, cin, tile), BF16),
                pltpu.VMEM((cout, 3 * cin), BF16),
                pltpu.VMEM((planes, rows, width), BF16),
                pltpu.VMEM((planes, rows, width), BF16),
                pltpu.VMEM((planes, 2, side, own, half), F32),
                pltpu.VMEM((planes, 2, side, own, half), F32),
                pltpu.VMEM((planes, 2, own, half), F32),
                pltpu.VMEM((planes, 2, own, half), F32),
                pltpu.VMEM((planes, 2, own, half), F32),
                pltpu.VMEM((planes, own, half), F32),
                pltpu.VMEM((8, half), F32),
                pltpu.VMEM((2 * n_inner, 8, half), F32),
                pltpu.VMEM((n_inner, own, half), F32),
                dma((planes,)),
                dma((planes, 2, side)),
                dma((planes, 2, side)),
                dma((planes,)),
                dma((planes,)),
                dma((2, n_inner)),
                dma((2 * n_inner,)),
                dma((planes,)),
                dma((n_inner,)),
                dma((planes, side)),
                dma((planes,)),
                dma((planes,)),
                dma((planes,)),
                dma((planes, 2)),
                dma((planes, 2)),
            ],
            compiler_params=pltpu.CompilerParams(
                collective_id=0, has_side_effects=True, vmem_limit_bytes=56 * 1024 * 1024
            ),
            name="adasum_step",
        )(inputs, cotangent, weight, momentum)
        input_grad, new_weight, new_momentum = pl.pallas_call(
            store_kernel,
            out_shape=tuple(
                jax.ShapeDtypeStruct(value.shape, F32) for value in (input_grad, new_weight, new_momentum)
            ),
            in_specs=[vmem] * 3,
            out_specs=(hbm, hbm, hbm),
            scratch_shapes=[dma((3,))],
            compiler_params=pltpu.CompilerParams(vmem_limit_bytes=4 * 1024 * 1024),
            name="store_results",
        )(input_grad, new_weight, new_momentum)
        return input_grad, new_weight.reshape(cout, half), new_momentum

    placed = (P(("outer", "inner"), None), P(("outer", "inner"), None), P(), P("inner", "outer"))
    return jax.shard_map(
        per_device,
        mesh=mesh,
        in_specs=placed,
        out_specs=(P(("outer", "inner"), None), P(None, "outer"), P("inner", "outer")),
        check_vma=False,
    )
```

```python
import functools

import jax
import jax.numpy as jnp
from jax import lax
from jax.experimental import pallas as pl
from jax.experimental.pallas import tpu as pltpu
from jax.sharding import PartitionSpec as P

MESH = pl.DeviceIdType.MESH
F32 = jnp.float32
BF16 = jnp.bfloat16


def split(value):
    high = value.astype(BF16)
    return high, (value - high.astype(F32)).astype(BF16)


def dot(a, b):
    return jnp.dot(a, b, preferred_element_type=F32)


def dot_t(a, b):
    return lax.dot_general(a, b, (((1,), (1,)), ((), ())), preferred_element_type=F32)


def row_tile(rows):
    best = 16
    for size in range(16, 257, 16):
        if rows % size == 0:
            best = size
    return best


def planes_of(inner):
    for planes in (4, 2):
        if inner % planes == 0:
            return planes
    return 1


def kernel(
    n_inner, planes, scale,
    x_ref, cot_hbm, w_ref, mom_ref,
    ig, nw_ref, nm_ref,
    cot, xcat, xt_hi, xt_lo, wcat, s_hi, s_lo, send1, recv1, send2, recv2, raw, moms, stat, stats, nw,
    cot_sem, ssem1, rsem1, ssem2, rsem2, ssem3, rsem3, ssem4, rsem4, ssem5, rsem5, ssem6, rsem6, ssem7, rsem7,
):
    o = lax.axis_index("outer")
    i = lax.axis_index("inner")
    side = n_inner // planes
    z = i // side
    j = i % side
    rows, cin = x_ref.shape
    cout = w_ref.shape[0]
    width = cout // planes
    own = cout // n_inner
    half = cin // 2
    tile = row_tile(rows)
    tiles = rows // tile

    def plane_of(c):
        return lax.rem(z + 1 + c, planes)

    def cot_copy(c):
        k = plane_of(c)
        return pltpu.make_async_copy(
            cot_hbm.at[:, pl.ds(pl.multiple_of(k * width, width), width)], cot.at[c], cot_sem.at[c]
        )

    for c in range(planes):
        cot_copy(c).start()

    barrier = pltpu.get_barrier_semaphore()
    n_all = 2 * n_inner

    for e in range(2):

        def greet(d, _, e=e):
            @pl.when((d + e) > 0)
            def _():
                pl.semaphore_signal(
                    barrier, inc=1,
                    device_id=(lax.rem(o + e, 2), lax.rem(i + d, n_inner)), device_id_type=MESH,
                )
            return 0

        lax.fori_loop(0, n_inner, greet, 0)

    for t in range(tiles):
        at = pl.ds(t * tile, tile)
        block = x_ref[at, :]
        high, low = split(block)
        xcat[at, 0:cin] = high
        xcat[at, cin : 2 * cin] = low
        xcat[at, 2 * cin : 3 * cin] = high
        block_t = block.T
        high_t, low_t = split(block_t)
        xt_hi[t] = high_t
        xt_lo[t] = low_t
    high, low = split(w_ref[...])
    wcat[:, 0:cin] = high
    wcat[:, cin : 2 * cin] = high
    wcat[:, 2 * cin : 3 * cin] = low

    def piece_copy(c, e, d):
        other = lax.rem(o + e, 2)
        target = lax.rem(j + d, side)
        return pltpu.make_async_remote_copy(
            src_ref=send1.at[c, other, target],
            dst_ref=recv1.at[c, o, j],
            send_sem=ssem1.at[c, e, d],
            recv_sem=rsem1.at[c, o, j],
            device_id=(other, z * side + target),
            device_id_type=MESH,
        )

    def piece_arrival(c, e, d):
        g = lax.rem(o + e, 2)
        source = lax.rem(j + side - d, side)
        return pltpu.make_async_remote_copy(
            src_ref=recv1.at[c, g, source],
            dst_ref=recv1.at[c, g, source],
            send_sem=ssem1.at[c, e, d],
            recv_sem=rsem1.at[c, g, source],
            device_id=(g, z * side + source),
            device_id_type=MESH,
        )

    pieces = [(e, d) for d in range(side) for e in range(2) if (e, d) != (0, 0)]

    def plane_copy(c):
        return pltpu.make_async_remote_copy(
            src_ref=send2.at[c],
            dst_ref=recv2.at[c],
            send_sem=ssem2.at[c],
            recv_sem=rsem2.at[c],
            device_id=(o, plane_of(c) * side + j),
            device_id_type=MESH,
        )

    def gather_plane(c):
        for e, d in pieces:
            piece_arrival(c, e, d).wait_recv()
        total = recv1[c, :, 0]
        for source in range(1, side):
            total = total + recv1[c, :, source]
        return total

    def line_copy(array, p, ssem, rsem):
        return pltpu.make_async_remote_copy(
            src_ref=array.at[z],
            dst_ref=array.at[z],
            send_sem=ssem.at[p],
            recv_sem=rsem.at[z],
            device_id=(o, lax.rem(z + p, planes) * side + j),
            device_id_type=MESH,
        )

    def line_arrival(array, p, ssem, rsem):
        source = lax.rem(z + planes - p, planes)
        return pltpu.make_async_remote_copy(
            src_ref=array.at[source],
            dst_ref=array.at[source],
            send_sem=ssem.at[p],
            recv_sem=rsem.at[source],
            device_id=(o, source * side + j),
            device_id_type=MESH,
        )

    moms[z] = mom_ref[...]
    far = planes // 2 if planes > 2 and planes % 2 == 0 else 0
    near = [p for p in range(1, planes) if p != far]

    def compute(c):
        k = plane_of(c)
        cot_copy(c).wait()
        w_at = pl.ds(pl.multiple_of(k * width, width), width)
        w_k = wcat[w_at, :]

        def pre_of(t):
            return dot_t(xcat[t * tile : (t + 1) * tile, :], w_k)

        pre_next = pre_of(0)
        acc = jnp.zeros((cin, width), F32)
        for t in range(tiles):
            pre = pre_next
            if t + 1 < tiles:
                pre_next = pre_of(t + 1)
            at = pl.ds(t * tile, tile)
            sig = 1.0 / (1.0 + jnp.exp(-pre))
            slope = cot[c, at, :] * (sig * (1.0 + pre * (1.0 - sig)))
            high, low = split(slope)
            s_hi[k, at, :] = high
            s_lo[k, at, :] = low
            acc = acc + (dot(xt_hi[t], high) + dot(xt_hi[t], low) + dot(xt_lo[t], high))
        grad = acc.T * scale
        for h in range(2):
            send1[c, h] = grad[:, h * half : (h + 1) * half].reshape(side, own, half)

    def chunk(c, _):
        compute(c)

        @pl.when(c == 0)
        def _():
            pl.semaphore_wait(barrier, n_all - 1)

        for e, d in pieces:
            piece_copy(c, e, d).start()
        recv1[c, o, j] = send1[c, o, j]

        @pl.when(c == 0)
        def _():
            for p in near:
                line_copy(moms, p, ssem6, rsem6).start()

        @pl.when(c > 0)
        def _():
            send2[c - 1] = gather_plane(c - 1)
            plane_copy(c - 1).start()

        return 0

    lax.fori_loop(0, planes, chunk, 0)

    def input_grad(t):
        at = pl.ds(t * tile, tile)
        total = jnp.zeros((tile, cin), F32)
        for k in range(planes):
            w_at = pl.ds(k * width, width)
            w_hi = wcat[w_at, 0:cin]
            total = total + dot(s_hi[k, at, :], w_hi) + dot(s_lo[k, at, :], w_hi)
            total = total + dot(s_hi[k, at, :], wcat[w_at, 2 * cin : 3 * cin])
        ig[at, :] = total

    early = tiles // 2 + 1
    for t in range(early):
        input_grad(t)

    total = gather_plane(planes - 1)
    for c in range(planes - 1):
        plane_copy(c).wait_recv()
        total = total + recv2[c]
    raw[z] = total
    first, second = total[0], total[1]

    me = o * n_inner + i
    rows_of = [
        jnp.sum(value, axis=0, keepdims=True)
        for value in (first * second, first * first, second * second)
    ]
    stat[...] = jnp.concatenate(rows_of + [jnp.zeros((5, half), F32)], axis=0)
    stats[me] = stat[...]

    def stat_copy(e, d):
        other = lax.rem(o + e, 2)
        target = lax.rem(i + d, n_inner)
        return pltpu.make_async_remote_copy(
            src_ref=stat,
            dst_ref=stats.at[me],
            send_sem=ssem3.at[e, d],
            recv_sem=rsem3.at[me],
            device_id=(other, target),
            device_id_type=MESH,
        )

    def stat_arrival(e, d):
        g = lax.rem(o + e, 2)
        source = lax.rem(i + n_inner - d, n_inner)
        return pltpu.make_async_remote_copy(
            src_ref=stat,
            dst_ref=stats.at[g * n_inner + source],
            send_sem=ssem3.at[e, d],
            recv_sem=rsem3.at[g * n_inner + source],
            device_id=(g, source),
            device_id_type=MESH,
        )

    everybody = [(e, d) for d in range(n_inner) for e in range(2) if (e, d) != (0, 0)]
    for e, d in everybody:
        stat_copy(e, d).start()
    for p in near:
        line_copy(raw, p, ssem4, rsem5).start()

    for t in range(early, tiles):
        input_grad(t)

    for e, d in everybody:
        stat_arrival(e, d).wait_recv()
    sums = jnp.sum(jnp.sum(stats[...], axis=0), axis=1, keepdims=True)
    cross, first_sq, second_sq = sums[0:1], sums[1:2], sums[2:3]
    first_by = 1.0 - cross / (2.0 * (first_sq + 1e-06))
    second_by = 1.0 - cross / (2.0 * (second_sq + 1e-06))

    def filter_copy(block, at, target, send_sem, recv_sem):
        return pltpu.make_async_remote_copy(
            src_ref=nw.at[block, at],
            dst_ref=nw.at[block, at],
            send_sem=send_sem,
            recv_sem=recv_sem,
            device_id=(o, z * side + target),
            device_id_type=MESH,
        )

    def far_copy(block):
        return pltpu.make_async_remote_copy(
            src_ref=nw.at[block],
            dst_ref=nw.at[block],
            send_sem=ssem4.at[far],
            recv_sem=rsem4.at[block],
            device_id=(o, lax.rem(z + far, planes) * side + j),
            device_id_type=MESH,
        )

    def plane_back(p):
        return lax.rem(z + planes - p, planes)

    whole = pl.ds(0, own)
    square = side == 4 and own % 16 == 0
    across = j + 1 - 2 * lax.rem(j, 2)
    along = j + 2 - 4 * (j // 2)
    targets = (across, along) if square else tuple(lax.rem(j + d, side) for d in range(1, side))
    sources = targets if square else tuple(lax.rem(j + side - d, side) for d in range(1, side))
    low_rows, high_rows = pl.ds(0, own // 2), pl.ds(own // 2, own // 2)

    def block_copies(p):
        block = plane_back(p) * side + j
        return [
            filter_copy(block, whole, target, ssem5.at[p, d], rsem4.at[block])
            for d, target in enumerate(targets)
        ]

    def block_arrival(p, d):
        block = plane_back(p) * side + sources[d]
        return filter_copy(block, whole, j, ssem5.at[p, d], rsem4.at[block])

    def forward_copies(p):
        q = plane_back(p)
        return [
            filter_copy(q * side + across, low_rows, along, ssem7.at[p, 0], rsem7.at[q, 0]),
            filter_copy(q * side + along, high_rows, across, ssem7.at[p, 1], rsem7.at[q, 1]),
        ]

    def forward(p):
        for d, copy in enumerate(forward_copies(p)):
            block_arrival(p, d).wait_recv()
            copy.start()

    order = [0]
    for p in range(1, planes // 2 + 1):
        order += [p] if p == planes - p else [p, planes - p]
    for at, p in enumerate(order):
        q = plane_back(p)
        block = q * side + j
        if p and p == far:
            far_copy(block).wait_recv()
        else:
            if p:
                line_arrival(moms, p, ssem6, rsem6).wait_recv()
                line_arrival(raw, p, ssem4, rsem5).wait_recv()
            momentum = 0.9 * moms[q] + (first_by * raw[q, 0] + second_by * raw[q, 1])
            if p == 0:
                nm_ref[...] = momentum
            w_rows = w_ref[pl.ds(pl.multiple_of(block * own, own), own), :]
            w_own = jnp.where(o == 0, w_rows[:, 0:half], w_rows[:, half : 2 * half])
            nw[block] = w_own - 0.1 * momentum
        if p == 0 and far:
            far_copy(block).start()
        for copy in block_copies(p):
            copy.start()
        if square and at:
            forward(order[at - 1])
    if square:
        forward(order[-1])
    for p in order:
        q = plane_back(p)
        if square:
            for d, at in enumerate((low_rows, high_rows)):
                filter_copy(q * side + (side - 1 - j), at, j, ssem7.at[p, d], rsem7.at[q, d]).wait_recv()
        else:
            for d in range(len(sources)):
                block_arrival(p, d).wait_recv()
    nw_ref[...] = nw[...]

    for c in range(planes):
        for e, d in pieces:
            piece_copy(c, e, d).wait_send()
        if c < planes - 1:
            plane_copy(c).wait_send()
    for e, d in everybody:
        stat_copy(e, d).wait_send()
    for p in range(planes):
        if p and p == far:
            far_copy(i).wait_send()
        elif p:
            line_copy(moms, p, ssem6, rsem6).wait_send()
            line_copy(raw, p, ssem4, rsem5).wait_send()
        for copy in block_copies(p):
            copy.wait_send()
        if square:
            for copy in forward_copies(p):
                copy.wait_send()


def store_kernel(a, b, c, a_out, b_out, c_out, sems):
    copies = [
        pltpu.make_async_copy(source, target, sems.at[n])
        for n, (source, target) in enumerate(((a, a_out), (b, b_out), (c, c_out)))
    ]
    for copy in copies:
        copy.start()
    for copy in copies:
        copy.wait()


def solution(mesh):
    n_inner = mesh.shape["inner"]
    planes = planes_of(n_inner)
    side = n_inner // planes

    def per_device(inputs, cotangent, weight, momentum):
        rows, cin = inputs.shape
        cout = weight.shape[0]
        own, half = momentum.shape
        width = cout // planes
        tile = row_tile(rows)
        tiles = rows // tile
        dma = pltpu.SemaphoreType.DMA
        vmem = pl.BlockSpec(memory_space=pltpu.VMEM)
        hbm = pl.BlockSpec(memory_space=pl.ANY)
        input_grad, new_weight, new_momentum = pl.pallas_call(
            functools.partial(kernel, n_inner, planes, 1.0 / (rows * n_inner)),
            out_shape=(
                pltpu.VMEM((rows, cin), F32),
                pltpu.VMEM((n_inner, own, half), F32),
                pltpu.VMEM((own, half), F32),
            ),
            in_specs=[vmem, hbm, vmem, vmem],
            out_specs=(vmem, vmem, vmem),
            scratch_shapes=[
                pltpu.VMEM((planes, rows, width), F32),
                pltpu.VMEM((rows, 3 * cin), BF16),
                pltpu.VMEM((tiles, cin, tile), BF16),
                pltpu.VMEM((tiles, cin, tile), BF16),
                pltpu.VMEM((cout, 3 * cin), BF16),
                pltpu.VMEM((planes, rows, width), BF16),
                pltpu.VMEM((planes, rows, width), BF16),
                pltpu.VMEM((planes, 2, side, own, half), F32),
                pltpu.VMEM((planes, 2, side, own, half), F32),
                pltpu.VMEM((planes, 2, own, half), F32),
                pltpu.VMEM((planes, 2, own, half), F32),
                pltpu.VMEM((planes, 2, own, half), F32),
                pltpu.VMEM((planes, own, half), F32),
                pltpu.VMEM((8, half), F32),
                pltpu.VMEM((2 * n_inner, 8, half), F32),
                pltpu.VMEM((n_inner, own, half), F32),
                dma((planes,)),
                dma((planes, 2, side)),
                dma((planes, 2, side)),
                dma((planes,)),
                dma((planes,)),
                dma((2, n_inner)),
                dma((2 * n_inner,)),
                dma((planes,)),
                dma((n_inner,)),
                dma((planes, side)),
                dma((planes,)),
                dma((planes,)),
                dma((planes,)),
                dma((planes, 2)),
                dma((planes, 2)),
            ],
            compiler_params=pltpu.CompilerParams(
                collective_id=0, has_side_effects=True, vmem_limit_bytes=56 * 1024 * 1024
            ),
            name="adasum_step",
        )(inputs, cotangent, weight, momentum)
        input_grad, new_weight, new_momentum = pl.pallas_call(
            store_kernel,
            out_shape=tuple(
                jax.ShapeDtypeStruct(value.shape, F32) for value in (input_grad, new_weight, new_momentum)
            ),
            in_specs=[vmem] * 3,
            out_specs=(hbm, hbm, hbm),
            scratch_shapes=[dma((3,))],
            compiler_params=pltpu.CompilerParams(vmem_limit_bytes=4 * 1024 * 1024),
            name="store_results",
        )(input_grad, new_weight, new_momentum)
        return input_grad, new_weight.reshape(cout, half), new_momentum

    placed = (P(("outer", "inner"), None), P(("outer", "inner"), None), P(), P("inner", "outer"))
    return jax.shard_map(
        per_device,
        mesh=mesh,
        in_specs=placed,
        out_specs=(P(("outer", "inner"), None), P(None, "outer"), P("inner", "outer")),
        check_vma=False,
    )
```
